32 devices in a mesh: data: 1 (over z), expert: 32 (over y, x, core).
Axes of the slice: x: 4, y: 4, z: 1, core: 2. Of those that a mesh axis runs over, the one named last changes fastest.
The devices are a block of a 4x4x8 slice.
Arguments:
- disp_one: bfloat16 [32, 64, 16, 2048], P('data', 'expert')
- slot_one: int32 [2048, 6], P(('data', 'expert'))
- expert_one: int32 [2048, 6], P(('data', 'expert'))
- gate_one: float32 [2048, 6], P(('data', 'expert'))
- disp_two: bfloat16 [32, 64, 16, 2048], P('data', 'expert')
- slot_two: int32 [2048, 6], P(('data', 'expert'))
- expert_two: int32 [2048, 6], P(('data', 'expert'))
- gate_two: float32 [2048, 6], P(('data', 'expert'))
- w_gate: bfloat16 [64, 2048, 1408], P('expert')
- w_up: bfloat16 [64, 2048, 1408], P('expert')
- w_down: bfloat16 [64, 1408, 2048], P('expert')
Outputs:
- output 1: bfloat16 [2048, 2048], P(('data', 'expert'))
- output 2: bfloat16 [2048, 2048], P(('data', 'expert'))
All inputs are finite; a program needn't handle non-finite values.
Results may differ from the reference program's by a relative error of at most 0.0015.
Values are sent between devices in bfloat16 or wider.
A program may use at most 768 MiB of HBM per device.

```python
import jax
import jax.numpy as jnp
from jax import lax

TOKENS_MB = 64
MODEL_DIM = 2048
FFN_DIM = 1408
EXPERTS = 64
TOP_K = 6
GROUP_SIZE = 32
CAPACITY = 16


def draw_routing(key):
    key_pop, key_hot, key_shift, key_noise = jax.random.split(key, 4)
    expert_ids = jnp.arange(EXPERTS, dtype=jnp.int32)
    popularity = jax.random.randint(key_pop, (EXPERTS,), 0, 48, dtype=jnp.int32)
    hot_expert = jax.random.randint(key_hot, (), 0, EXPERTS, dtype=jnp.int32)
    shift_by = jax.random.randint(key_shift, (), 0, EXPERTS, dtype=jnp.int32)
    noise_int = jax.random.randint(key_noise, (GROUP_SIZE, TOKENS_MB, EXPERTS), 0, 64, dtype=jnp.int32)
    src_ids = jnp.arange(GROUP_SIZE, dtype=jnp.int32)[:, None]
    tok_ids = jnp.arange(TOKENS_MB, dtype=jnp.int32)[None, :]
    forced = (tok_ids + src_ids + shift_by) % EXPERTS
    scores = (popularity + noise_int
              + 4096 * (expert_ids == hot_expert).astype(jnp.int32)
              + 2048 * (expert_ids == forced[:, :, None]).astype(jnp.int32))
    _, chosen = lax.top_k(scores * EXPERTS + expert_ids, TOP_K)
    chosen = chosen.astype(jnp.int32)
    one_hot = (chosen[:, :, :, None] == expert_ids).astype(jnp.int32)
    one_hot = one_hot.reshape(GROUP_SIZE, TOKENS_MB * TOP_K, EXPERTS)
    position = jnp.sum((jnp.cumsum(one_hot, axis=1) - 1) * one_hot, axis=-1)
    slot_ids = jnp.where(position < CAPACITY, position, -1)
    return (slot_ids.reshape(GROUP_SIZE * TOKENS_MB, TOP_K).astype(jnp.int32),
            chosen.reshape(GROUP_SIZE * TOKENS_MB, TOP_K))


def draw_gates(key):
    logits = 0.8 * jax.random.normal(key, (GROUP_SIZE * TOKENS_MB, TOP_K), jnp.float32)
    return jax.nn.softmax(logits, axis=-1)


def setup_inputs(seed: int = 0, part: int = 0) -> dict:
    base_key = jax.random.key(seed)
    part_keys = jax.random.split(jax.random.fold_in(base_key, part), 6)
    weight_keys = jax.random.split(base_key, 3)
    disp_shape = (GROUP_SIZE, EXPERTS, CAPACITY, MODEL_DIM)
    disp_one = jax.random.normal(part_keys[0], disp_shape, jnp.float32).astype(jnp.bfloat16)
    slot_one, expert_one = draw_routing(part_keys[1])
    gate_one = draw_gates(part_keys[2])
    disp_two = jax.random.normal(part_keys[3], disp_shape, jnp.float32).astype(jnp.bfloat16)
    slot_two, expert_two = draw_routing(part_keys[4])
    gate_two = draw_gates(part_keys[5])
    w_gate = (jax.random.normal(weight_keys[0], (EXPERTS, MODEL_DIM, FFN_DIM), jnp.float32) * MODEL_DIM ** -0.5).astype(jnp.bfloat16)
    w_up = (jax.random.normal(weight_keys[1], (EXPERTS, MODEL_DIM, FFN_DIM), jnp.float32) * MODEL_DIM ** -0.5).astype(jnp.bfloat16)
    w_down = (jax.random.normal(weight_keys[2], (EXPERTS, FFN_DIM, MODEL_DIM), jnp.float32) * FFN_DIM ** -0.5).astype(jnp.bfloat16)
    return {'disp_one': disp_one, 'slot_one': slot_one, 'expert_one': expert_one, 'gate_one': gate_one,
            'disp_two': disp_two, 'slot_two': slot_two, 'expert_two': expert_two, 'gate_two': gate_two,
            'w_gate': w_gate, 'w_up': w_up, 'w_down': w_down}


def expert_outputs(disp, w_gate, w_up, w_down):
    rows = jnp.swapaxes(disp, 0, 1).reshape(EXPERTS, GROUP_SIZE * CAPACITY, MODEL_DIM)

    def one_expert(operands):
        x_rows, gate_mat, up_mat, down_mat = operands
        gate_act = jnp.dot(x_rows, gate_mat, preferred_element_type=jnp.float32)
        up_act = jnp.dot(x_rows, up_mat, preferred_element_type=jnp.float32)
        hidden = (jax.nn.silu(gate_act) * up_act).astype(jnp.bfloat16)
        return jnp.dot(hidden, down_mat, preferred_element_type=jnp.float32).astype(jnp.bfloat16)

    return lax.map(one_expert, (rows, w_gate, w_up, w_down))


def combine(expert_rows, slot_ids, expert_ids, gates):
    y_all = expert_rows.reshape(EXPERTS, GROUP_SIZE, CAPACITY, MODEL_DIM)
    source = jnp.arange(GROUP_SIZE * TOKENS_MB, dtype=jnp.int32) // TOKENS_MB
    kept = jnp.where(slot_ids >= 0, gates, 0.0)
    safe_slot = jnp.maximum(slot_ids, 0)
    total = jnp.zeros((GROUP_SIZE * TOKENS_MB, MODEL_DIM), jnp.float32)
    for choice in range(TOP_K):
        picked = y_all[expert_ids[:, choice], source, safe_slot[:, choice]]
        total = total + kept[:, choice, None] * picked.astype(jnp.float32)
    return total.astype(jnp.bfloat16)


def reference(disp_one, slot_one, expert_one, gate_one, disp_two, slot_two, expert_two, gate_two, w_gate, w_up, w_down):
    out_one = combine(expert_outputs(disp_one, w_gate, w_up, w_down), slot_one, expert_one, gate_one)
    out_two = combine(expert_outputs(disp_two, w_gate, w_up, w_down), slot_two, expert_two, gate_two)
    return (out_one, out_two)
```

```python
import functools
import math

import jax
import jax.numpy as jnp
from jax import lax
from jax.experimental import pallas as pl
from jax.experimental.pallas import tpu as pltpu
from jax.sharding import PartitionSpec as P

MESH = pl.DeviceIdType.MESH
AXIS = 'expert'
CORES = 2
BF16_MAX = 3.3895313892515355e38
NT = 256
DN = 512


def moe_kernel(side, top_k, disp_one, disp_two, meta_one, meta_two, w_gate, w_up, w_down, out_one, out_two,
               wgu, wd, stage, recv, hid, meta, part, relay, final,
               x_sem, w_sem, d_sem, send_sem, recv_sem, meta_send, meta_recv,
               part_send, relay_recv, final_recv):
    n_exp, dim, ffn = w_gate.shape
    cap = disp_one.shape[-2]
    half = dim // 2
    tokens = out_one.shape[0]
    rows = 2 * side * CORES * cap
    group = side * CORES * n_exp * cap
    n_main = ffn // NT
    tail = ffn - n_main * NT
    metas, disps, outs = (meta_one, meta_two), (disp_one, disp_two), (out_one, out_two)

    me = lax.axis_index(AXIS)
    c = me % CORES
    x = (me // CORES) % side
    y = me // (CORES * side)

    def dev(yy, xx, cc):
        return {AXIS: ((yy % side) * side + (xx % side)) * CORES + cc % CORES}

    def along(m, first, step, dc):
        if (m == 0) == first:
            return dev(y, x + step, c + dc)
        return dev(y + step, x, c + dc)

    def rel(it):
        return (2 - it + (it // 2) * (2 * it - 1)) % side

    def load_rows(u, it, e):
        r = rel(it)
        pltpu.make_async_copy(disp_one.at[(y + r) % side, :, e], stage.at[u, 0], x_sem.at[u, 0]).start()
        for k in range(side):
            pltpu.make_async_copy(disp_two.at[k, pl.ds((x + r) % side * CORES, CORES), e],
                                  stage.at[u, 1, k * CORES:(k + 1) * CORES], x_sem.at[u, 1]).start()

    def wait_rows(u):
        for m in range(2):
            pltpu.make_async_copy(stage.at[u, m], stage.at[u, m], x_sem.at[u, m]).wait()

    def load_weights(e):
        for j in range(n_main):
            for k, w in enumerate((w_gate, w_up)):
                pltpu.make_async_copy(w.at[e, :, pl.ds(j * NT, NT)], wgu.at[e, :, pl.ds((2 * j + k) * NT, NT)],
                                      w_sem.at[e, 2 * j + k]).start()
        for k, w in enumerate((w_gate, w_up)):
            pltpu.make_async_copy(w.at[e, :, pl.ds(n_main * NT, tail)],
                                  wgu.at[e, :, pl.ds(2 * n_main * NT + k * tail, tail)],
                                  w_sem.at[e, 2 * n_main + k]).start()
        for j in range(dim // DN):
            pltpu.make_async_copy(w_down.at[e, :, pl.ds(j * DN, DN)], wd.at[e, :, pl.ds(j * DN, DN)],
                                  d_sem.at[e, j]).start()

    def wait_gu(e, j):
        width = NT if j < n_main else tail
        for k in range(2):
            ref = wgu.at[e, :, pl.ds(2 * j * NT + k * width, width)]
            pltpu.make_async_copy(ref, ref, w_sem.at[e, 2 * j + k]).wait()

    def wait_down(e, j):
        ref = wd.at[e, :, pl.ds(j * DN, DN)]
        pltpu.make_async_copy(ref, ref, d_sem.at[e, j]).wait()

    def unit(u, e, first):
        wait_rows(u)
        for j in range(n_main + 1):
            width = NT if j < n_main else tail
            if first:
                wait_gu(e, j)
            both = jnp.dot(stage[u].reshape(rows, dim), wgu[e, :, 2 * j * NT:2 * j * NT + 2 * width],
                           preferred_element_type=jnp.float32)
            gate_act, up_act = both[:, :width], both[:, width:]
            hid[:, j * NT:j * NT + width] = (gate_act * jax.nn.sigmoid(gate_act) * up_act).astype(jnp.bfloat16)
        for j in range(dim // DN):
            if first:
                wait_down(e, j)
            y_rows = jnp.dot(hid[...], wd[e, :, j * DN:(j + 1) * DN], preferred_element_type=jnp.float32)
            y_rows = jnp.where(jnp.abs(y_rows) <= BF16_MAX, y_rows, 0.0).astype(jnp.bfloat16)
            stage[u, :, :, :, j * DN:(j + 1) * DN] = y_rows.reshape(2, side * CORES, cap, DN)

    hops = [(2, 0), (2, 1), (1, 0), (side - 1, 0), (1, 1), (side - 1, 1), (0, 1)]

    def send_unit(u, it, e):
        for step, dc in hops:
            for m in range(2):
                pos = x if m == 0 else y
                pltpu.make_async_remote_copy(
                    src_ref=stage.at[u, m, (pos + step) % side * CORES + (c + dc) % CORES],
                    dst_ref=recv.at[m, it, pos, c, e],
                    send_sem=send_sem.at[u, m], recv_sem=recv_sem.at[m, it],
                    device_id=along(m, True, step, dc), device_id_type=MESH).start()
        for m in range(2):
            pos = x if m == 0 else y
            pltpu.make_async_copy(stage.at[u, m, pos * CORES + c], recv.at[m, it, pos, c, e], recv_sem.at[m, it]).start()

    def combine(m, it, meta_tile):
        ref = recv.at[m, it]
        pltpu.make_async_copy(ref, ref, recv_sem.at[m, it]).wait()
        lane = lax.broadcasted_iota(jnp.int32, (tokens, group), 1)
        if m == 0:
            row_id = lane + y * group
        else:
            sub = CORES * n_exp * cap
            row_id = (lane // sub) * group + x * sub + lane % sub
        row_id = row_id.astype(jnp.float32)
        mix = jnp.zeros((tokens, group), jnp.float32)
        for j in range(top_k):
            mix = jnp.where(meta_tile[:, j:j + 1] == row_id, meta_tile[:, top_k + j:top_k + j + 1], mix)
        high = mix.astype(jnp.bfloat16)
        rest = mix - high.astype(jnp.float32)
        mid = rest.astype(jnp.bfloat16)
        low = (rest - mid.astype(jnp.float32)).astype(jnp.bfloat16)
        mix3 = jnp.concatenate([high, mid, low], axis=0)
        for j in range(dim // DN):
            table = recv[m, it, :, :, :, :, j * DN:(j + 1) * DN].reshape(group, DN)
            prod = jnp.dot(mix3, table, preferred_element_type=jnp.float32)
            total = prod[2 * tokens:] + prod[tokens:2 * tokens] + prod[:tokens]
            h, off = (j * DN) // half, (j * DN) % half
            part[m, it, h, :, off:off + DN] = total

    def wait_meta(m, it):
        ref = meta.at[m, it]
        pltpu.make_async_copy(ref, ref, meta_recv.at[m, it]).wait()

    load_rows(0, 0, 0)
    load_weights(0)
    load_rows(1, 0, 1)
    load_weights(1)

    barrier = pltpu.get_barrier_semaphore()
    peers = 0
    for step in range(side):
        for dc in range(CORES):
            if (step, dc) != (0, 0):
                pl.semaphore_signal(barrier, inc=1, device_id=along(0, True, step, dc), device_id_type=MESH)
                peers += 1
            if step != 0:
                pl.semaphore_signal(barrier, inc=1, device_id=along(1, True, step, dc), device_id_type=MESH)
                peers += 1

    def load_rest(u, carry):
        load_rows(u, u // n_exp, u % n_exp)
        return carry

    lax.fori_loop(n_exp, side * n_exp, load_rest, 0)
    pl.semaphore_wait(barrier, peers)

    for m in range(2):
        for it in range(side - 1):
            step = side - (2, 1, 3)[it]
            pltpu.make_async_remote_copy(src_ref=metas[m], dst_ref=meta.at[m, it], send_sem=meta_send.at[m, it],
                                         recv_sem=meta_recv.at[m, it], device_id=along(m, False, step, 0),
                                         device_id_type=MESH).start()

    for e in range(n_exp):
        unit(e, e, True)
        send_unit(e, 0, e)

    def send_far(m):
        for h, step in ((0, 1), (1, side - 1)):
            pltpu.make_async_remote_copy(src_ref=part.at[m, 0, h], dst_ref=relay.at[m, h],
                                         send_sem=part_send.at[m, h], recv_sem=relay_recv.at[m, h],
                                         device_id=along(m, False, step, 0), device_id_type=MESH).start()

    def body(it, carry):
        for e in range(n_exp):
            u = it * n_exp + e
            unit(u, e, False)
            send_unit(u, it, e)

        @pl.when(it < side - 1)
        def _():
            for m in range(2):
                @pl.when(it == 1)
                def _():
                    wait_meta(m, 0)

                @pl.when(it == 2)
                def _():
                    wait_meta(m, 1)
                combine(m, it - 1, meta[m, it - 1])

            @pl.when(it == 1)
            def _():
                for m in range(2):
                    send_far(m)
        return carry

    lax.fori_loop(1, side, body, 0)

    def send_near(m, it):
        h = it - 1
        step = (1, side - 1)[h]
        ref = relay.at[m, h]
        pltpu.make_async_copy(ref, ref, relay_recv.at[m, h]).wait()
        part[m, it, h] = part[m, it, h] + relay[m, h]
        pltpu.make_async_remote_copy(src_ref=part.at[m, it], dst_ref=final.at[m, h],
                                     send_sem=part_send.at[m, 2 + h], recv_sem=final_recv.at[m, h],
                                     device_id=along(m, False, step, 0), device_id_type=MESH).start()

    for m in range(2):
        send_near(m, 1)
    for m in range(2):
        wait_meta(m, 2)
        combine(m, 2, meta[m, 2])
        send_near(m, 2)
    for m in range(2):
        combine(m, 3, metas[m][...])
    for m in range(2):
        for h in range(2):
            ref = final.at[m, h]
            pltpu.make_async_copy(ref, ref, final_recv.at[m, h]).wait()
        for h in range(2):
            total = part[m, 3, h] + final[m, 0, h] + final[m, 1, h]
            outs[m][:, h * half:(h + 1) * half] = total.astype(jnp.bfloat16)

    def drain(u, carry):
        for m in range(2):
            ref = stage.at[u, m, pl.ds(0, side * CORES - 1)]
            pltpu.make_async_copy(ref, ref, send_sem.at[u, m]).wait()
        return carry

    lax.fori_loop(0, side * n_exp, drain, 0)
    for m in range(2):
        for it in range(side - 1):
            pltpu.make_async_copy(metas[m], metas[m], meta_send.at[m, it]).wait()
        for h in range(2):
            ref = part.at[m, 0, h]
            pltpu.make_async_copy(ref, ref, part_send.at[m, h]).wait()
            ref = part.at[m, 1 + h]
            pltpu.make_async_copy(ref, ref, part_send.at[m, 2 + h]).wait()


def solution(mesh):
    members = mesh.shape[AXIS]
    side = math.isqrt(members // CORES)
    disp_spec = P('data', 'expert', None, None)
    tok_spec = P(('data', 'expert'), None)
    weight_spec = P('expert', None, None)

    def local_step(disp_one, slot_one, expert_one, gate_one, disp_two, slot_two, expert_two, gate_two, w_gate, w_up, w_down):
        _, n_exp, cap, dim = disp_one.shape
        tokens, top_k = slot_one.shape
        ffn = w_gate.shape[-1]
        units = side * n_exp

        def pack(slot_ids, expert_ids, gates):
            rows = jnp.where(slot_ids >= 0, expert_ids * cap + slot_ids, -1).astype(jnp.float32)
            return jnp.pad(jnp.concatenate([rows, gates], axis=1), ((0, 0), (0, 128 - 2 * top_k)))

        split = (side, side * CORES, n_exp, cap, dim)
        any_spec = pl.BlockSpec(memory_space=pl.ANY)
        vmem_spec = pl.BlockSpec(memory_space=pltpu.VMEM)
        dma = pltpu.SemaphoreType.DMA
        flops = 2 * 2 * members * n_exp * cap * dim * ffn * 3
        return pl.pallas_call(
            functools.partial(moe_kernel, side, top_k),
            out_shape=(jax.ShapeDtypeStruct((tokens, dim), jnp.bfloat16),) * 2,
            in_specs=[any_spec, any_spec, vmem_spec, vmem_spec, any_spec, any_spec, any_spec],
            out_specs=(vmem_spec, vmem_spec),
            scratch_shapes=[
                pltpu.VMEM((n_exp, dim, 2 * ffn), jnp.bfloat16),
                pltpu.VMEM((n_exp, ffn, dim), jnp.bfloat16),
                pltpu.VMEM((units, 2, side * CORES, cap, dim), jnp.bfloat16),
                pltpu.VMEM((2, side, side, CORES, n_exp, cap, dim), jnp.bfloat16),
                pltpu.VMEM((2 * side * CORES * cap, ffn), jnp.bfloat16),
                pltpu.VMEM((2, side - 1, tokens, 128), jnp.float32),
                pltpu.VMEM((2, side, 2, tokens, dim // 2), jnp.float32),
                pltpu.VMEM((2, 2, tokens, dim // 2), jnp.float32),
                pltpu.VMEM((2, 2, 2, tokens, dim // 2), jnp.float32),
                dma((units, 2)), dma((n_exp, 2 * (ffn // NT) + 2)), dma((n_exp, dim // DN)),
                dma((units, 2)), dma((2, side)), dma((2, side - 1)), dma((2, side - 1)),
                dma((2, 4)), dma((2, 2)), dma((2, 2)),
            ],
            compiler_params=pltpu.CompilerParams(collective_id=0, has_side_effects=True,
                                                 vmem_limit_bytes=67_043_328),
            cost_estimate=pl.CostEstimate(flops=flops, bytes_accessed=43_000_000, transcendentals=0),
        )(disp_one.reshape(split), disp_two.reshape(split), pack(slot_one, expert_one, gate_one),
          pack(slot_two, expert_two, gate_two), w_gate, w_up, w_down)

    in_specs = (disp_spec, tok_spec, tok_spec, tok_spec, disp_spec, tok_spec, tok_spec, tok_spec,
                weight_spec, weight_spec, weight_spec)
    return jax.shard_map(local_step, mesh=mesh, in_specs=in_specs, out_specs=(tok_spec, tok_spec), check_vma=False)
```

```python
import functools
import math

import jax
import jax.numpy as jnp
from jax import lax
from jax.experimental import pallas as pl
from jax.experimental.pallas import tpu as pltpu
from jax.sharding import PartitionSpec as P

MESH = pl.DeviceIdType.MESH
AXIS = 'expert'
CORES = 2
BF16_MAX = 3.3895313892515355e38
NT = 512
DN = 512
LANES = 128


def moe_kernel(side, disp_one, disp_two, slot_one, slot_two, expert_one, expert_two, gate_one, gate_two, w_gate, w_up, w_down, out_one, out_two,
               wgu, wd, stage, recv, hid, own, meta, part, relay, final,
               x_sem, w_sem, d_sem, send_sem, recv_sem, meta_send, meta_recv,
               part_send, relay_recv, final_recv):
    n_exp, dim, ffn = w_gate.shape
    cap = disp_one.shape[-2]
    half = dim // 2
    tokens = out_one.shape[0]
    rows = 2 * side * CORES * cap
    group = side * CORES * n_exp * cap
    n_main = ffn // NT
    tail = ffn - n_main * NT
    routes = ((slot_one, expert_one, gate_one), (slot_two, expert_two, gate_two))
    outs = (out_one, out_two)
    top_k = slot_one.shape[0]
    top_row = 8

    me = lax.axis_index(AXIS)
    c = me % CORES
    x = (me // CORES) % side
    y = me // (CORES * side)
    turn = 1 - 2 * c

    def dev(yy, xx, cc):
        return {AXIS: ((yy % side) * side + (xx % side)) * CORES + cc % CORES}

    def along(m, first, step, dc):
        if (m == 0) == first:
            return dev(y, x + step, c + dc)
        return dev(y + step, x, c + dc)

    def rel(it):
        return (2 - it + (it // 2) * (2 * it - 1)) % side

    def load_rows(u, it, e):
        for k in range(CORES):
            r = (1 - 2 * k) * rel(it) + side
            pltpu.make_async_copy(disp_one.at[(y + r) % side, :, k, e], stage.at[u, 0, pl.ds(k * side, side)], x_sem.at[u, 0]).start()
            pltpu.make_async_copy(disp_two.at[:, (x + r) % side, k, e], stage.at[u, 1, pl.ds(k * side, side)], x_sem.at[u, 1]).start()

    def wait_rows(u):
        for m in range(2):
            pltpu.make_async_copy(stage.at[u, m], stage.at[u, m], x_sem.at[u, m]).wait()

    def load_weights(e):
        for j in range(n_main):
            for k, w in enumerate((w_gate, w_up)):
                pltpu.make_async_copy(w.at[e, :, pl.ds(j * NT, NT)], wgu.at[e, :, pl.ds((2 * j + k) * NT, NT)],
                                      w_sem.at[e, 2 * j + k]).start()
        for k, w in enumerate((w_gate, w_up)):
            pltpu.make_async_copy(w.at[e, :, pl.ds(n_main * NT, tail)],
                                  wgu.at[e, :, pl.ds(2 * n_main * NT + k * tail, tail)],
                                  w_sem.at[e, 2 * n_main + k]).start()
        for j in range(dim // DN):
            pltpu.make_async_copy(w_down.at[e, :, pl.ds(j * DN, DN)], wd.at[e, :, pl.ds(j * DN, DN)],
                                  d_sem.at[e, j]).start()

    def wait_gu(e, j):
        width = NT if j < n_main else tail
        for k in range(2):
            ref = wgu.at[e, :, pl.ds(2 * j * NT + k * width, width)]
            pltpu.make_async_copy(ref, ref, w_sem.at[e, 2 * j + k]).wait()

    def wait_down(e, j):
        ref = wd.at[e, :, pl.ds(j * DN, DN)]
        pltpu.make_async_copy(ref, ref, d_sem.at[e, j]).wait()

    def hidden(j, both):
        width = NT if j < n_main else tail
        gate_act, up_act = both[:, :width], both[:, width:]
        hid[:, j * NT:j * NT + width] = (gate_act * jax.nn.sigmoid(gate_act) * up_act).astype(jnp.bfloat16)

    def put_rows(u, j, width, y_rows):
        y_rows = jnp.where(jnp.abs(y_rows) <= BF16_MAX, y_rows, 0.0).astype(jnp.bfloat16)
        stage[u, :, :, :, j * width:(j + 1) * width] = y_rows.reshape(2, CORES * side, cap, width)

    def dot(a, b):
        return jnp.dot(a, b, preferred_element_type=jnp.float32)

    def first_unit(u, e):
        wait_rows(u)
        for j in range(n_main + 1):
            width = NT if j < n_main else tail
            wait_gu(e, j)
            hidden(j, dot(stage[u].reshape(rows, dim), wgu[e, :, 2 * j * NT:2 * j * NT + 2 * width]))
        for j in range(dim // DN):
            wait_down(e, j)
            put_rows(u, j, DN, dot(hid[...], wd[e, :, j * DN:(j + 1) * DN]))

    def unit(u, e):
        wait_rows(u)
        both = dot(stage[u].reshape(rows, dim), wgu[e])
        for j in range(n_main + 1):
            width = NT if j < n_main else tail
            hidden(j, both[:, 2 * j * NT:2 * j * NT + 2 * width])
        put_rows(u, 0, dim, dot(hid[...], wd[e]))

    hops = [(2, 0), (2, 1), (1, 0), (side - 1, 0), (1, 1), (side - 1, 1), (0, 1)]

    def send_unit(u, it, e):
        for step, dc in hops:
            for m in range(2):
                pos = x if m == 0 else y
                pltpu.make_async_remote_copy(
                    src_ref=stage.at[u, m, (c + dc) % CORES * side + (pos + step) % side],
                    dst_ref=recv.at[m, it, pos, c, e],
                    send_sem=send_sem.at[u, m], recv_sem=recv_sem.at[m, it],
                    device_id=along(m, True, step, dc), device_id_type=MESH).start()
        for m in range(2):
            pos = x if m == 0 else y
            pltpu.make_async_copy(stage.at[u, m, c * side + pos], recv.at[m, it, pos, c, e], recv_sem.at[m, it]).start()

    def combine(m, it, meta_tile):
        ref = recv.at[m, it]
        pltpu.make_async_copy(ref, ref, recv_sem.at[m, it]).wait()
        lane = lax.broadcasted_iota(jnp.int32, (tokens, group), 1)
        if m == 0:
            row_id = lane + y * group
        else:
            sub = CORES * n_exp * cap
            row_id = (lane // sub) * group + x * sub + lane % sub
        row_id = row_id.astype(jnp.float32)
        table = jnp.transpose(meta_tile)
        mix = jnp.zeros((tokens, group), jnp.float32)
        for j in range(top_k):
            mix = jnp.where(table[:tokens, j:j + 1] == row_id, table[:tokens, top_row + j:top_row + j + 1], mix)
        high = mix.astype(jnp.bfloat16)
        rest = mix - high.astype(jnp.float32)
        mid = rest.astype(jnp.bfloat16)
        low = (rest - mid.astype(jnp.float32)).astype(jnp.bfloat16)
        mix3 = jnp.concatenate([high, mid, low], axis=0)
        for j in range(dim // DN):
            prod = dot(mix3, recv[m, it, :, :, :, :, j * DN:(j + 1) * DN].reshape(group, DN))
            total = prod[2 * tokens:] + prod[tokens:2 * tokens] + prod[:tokens]
            h, off = (j * DN) // half, (j * DN) % half
            part[m, it, h, :, off:off + DN] = total

    def wait_meta(m, it):
        ref = meta.at[m, it]
        pltpu.make_async_copy(ref, ref, meta_recv.at[m, it]).wait()

    load_rows(0, 0, 0)
    load_weights(0)
    load_rows(1, 0, 1)
    load_weights(1)

    barrier = pltpu.get_barrier_semaphore()
    peers = 0
    for step in range(side):
        for dc in range(CORES):
            if (step, dc) != (0, 0):
                pl.semaphore_signal(barrier, inc=1, device_id=along(0, True, step, dc), device_id_type=MESH)
                peers += 1
            if step != 0:
                pl.semaphore_signal(barrier, inc=1, device_id=along(1, True, step, dc), device_id_type=MESH)
                peers += 1

    def load_rest(u, carry):
        load_rows(u, u // n_exp, u % n_exp)
        return carry

    lax.fori_loop(n_exp, side * n_exp, load_rest, 0)
    for m, (slots, experts, gates) in enumerate(routes):
        own[m] = jnp.zeros((2 * top_row, LANES), jnp.float32)
        kept = slots[...] >= 0
        own[m, :top_k, :tokens] = jnp.where(kept, experts[...] * cap + slots[...], -1).astype(jnp.float32)
        own[m, top_row:top_row + top_k, :tokens] = gates[...]
    pl.semaphore_wait(barrier, peers)

    for m in range(2):
        for it in range(side - 1):
            step = side - turn * (2, 1, 3)[it]
            pltpu.make_async_remote_copy(src_ref=own.at[m], dst_ref=meta.at[m, it], send_sem=meta_send.at[m, it],
                                         recv_sem=meta_recv.at[m, it], device_id=along(m, False, step, 0),
                                         device_id_type=MESH).start()

    for e in range(n_exp):
        first_unit(e, e)
        send_unit(e, 0, e)

    def send_far(m):
        for h, step in ((0, side + turn), (1, side - turn)):
            pltpu.make_async_remote_copy(src_ref=part.at[m, 0, h], dst_ref=relay.at[m, h],
                                         send_sem=part_send.at[m, h], recv_sem=relay_recv.at[m, h],
                                         device_id=along(m, False, step, 0), device_id_type=MESH).start()

    def send_near(m, it):
        h = it - 1
        step = side + (turn, -turn)[h]
        ref = relay.at[m, h]
        pltpu.make_async_copy(ref, ref, relay_recv.at[m, h]).wait()
        part[m, it, h] = part[m, it, h] + relay[m, h]
        pltpu.make_async_remote_copy(src_ref=part.at[m, it], dst_ref=final.at[m, h],
                                     send_sem=part_send.at[m, 2 + h], recv_sem=final_recv.at[m, h],
                                     device_id=along(m, False, step, 0), device_id_type=MESH).start()

    def body(it, carry):
        for e in range(n_exp):
            u = it * n_exp + e
            unit(u, e)
            send_unit(u, it, e)

        @pl.when(it < side - 1)
        def _():
            for m in range(2):
                @pl.when(it == 1)
                def _():
                    wait_meta(m, 0)

                @pl.when(it == 2)
                def _():
                    wait_meta(m, 1)
                combine(m, it - 1, meta[m, it - 1])

            @pl.when(it == 1)
            def _():
                for m in range(2):
                    send_far(m)

            @pl.when(it == 2)
            def _():
                for m in range(2):
                    send_near(m, 1)
        return carry

    lax.fori_loop(1, side, body, 0)
    for m in range(2):
        wait_meta(m, 2)
        combine(m, 2, meta[m, 2])
        send_near(m, 2)
    for m in range(2):
        combine(m, 3, own[m])
    for m in range(2):
        for h in range(2):
            ref = final.at[m, h]
            pltpu.make_async_copy(ref, ref, final_recv.at[m, h]).wait()
        for h in range(2):
            total = part[m, 3, h] + final[m, 0, h] + final[m, 1, h]
            outs[m][:, h * half:(h + 1) * half] = total.astype(jnp.bfloat16)

    def drain(u, carry):
        for m in range(2):
            ref = stage.at[u, m, pl.ds(0, side * CORES - 1)]
            pltpu.make_async_copy(ref, ref, send_sem.at[u, m]).wait()
        return carry

    lax.fori_loop(0, side * n_exp, drain, 0)
    for m in range(2):
        for it in range(side - 1):
            pltpu.make_async_copy(own.at[m], own.at[m], meta_send.at[m, it]).wait()
        for h in range(2):
            ref = part.at[m, 0, h]
            pltpu.make_async_copy(ref, ref, part_send.at[m, h]).wait()
            ref = part.at[m, 1 + h]
            pltpu.make_async_copy(ref, ref, part_send.at[m, 2 + h]).wait()


def solution(mesh):
    members = mesh.shape[AXIS]
    side = math.isqrt(members // CORES)
    disp_spec = P('data', 'expert', None, None)
    tok_spec = P(('data', 'expert'), None)
    weight_spec = P('expert', None, None)

    def local_step(disp_one, slot_one, expert_one, gate_one, disp_two, slot_two, expert_two, gate_two, w_gate, w_up, w_down):
        _, n_exp, cap, dim = disp_one.shape
        tokens = slot_one.shape[0]
        ffn = w_gate.shape[-1]
        units = side * n_exp

        split = (side, side, CORES, n_exp, cap, dim)
        any_spec = pl.BlockSpec(memory_space=pl.ANY)
        vmem_spec = pl.BlockSpec(memory_space=pltpu.VMEM)
        dma = pltpu.SemaphoreType.DMA
        flops = 2 * 2 * members * n_exp * cap * dim * ffn * 3
        return pl.pallas_call(
            functools.partial(moe_kernel, side),
            out_shape=(jax.ShapeDtypeStruct((tokens, dim), jnp.bfloat16),) * 2,
            in_specs=[any_spec] * 2 + [vmem_spec] * 6 + [any_spec] * 3,
            out_specs=(vmem_spec, vmem_spec),
            scratch_shapes=[
                pltpu.VMEM((n_exp, dim, 2 * ffn), jnp.bfloat16),
                pltpu.VMEM((n_exp, ffn, dim), jnp.bfloat16),
                pltpu.VMEM((units, 2, CORES * side, cap, dim), jnp.bfloat16),
                pltpu.VMEM((2, side, side, CORES, n_exp, cap, dim), jnp.bfloat16),
                pltpu.VMEM((2 * side * CORES * cap, ffn), jnp.bfloat16),
                pltpu.VMEM((2, 16, LANES), jnp.float32),
                pltpu.VMEM((2, side - 1, 16, LANES), jnp.float32),
                pltpu.VMEM((2, side, 2, tokens, dim // 2), jnp.float32),
                pltpu.VMEM((2, 2, tokens, dim // 2), jnp.float32),
                pltpu.VMEM((2, 2, 2, tokens, dim // 2), jnp.float32),
                dma((units, 2)), dma((n_exp, 2 * (ffn // NT) + 2)), dma((n_exp, dim // DN)),
                dma((units, 2)), dma((2, side)), dma((2, side - 1)), dma((2, side - 1)),
                dma((2, 4)), dma((2, 2)), dma((2, 2)),
            ],
            compiler_params=pltpu.CompilerParams(collective_id=0, has_side_effects=True,
                                                 vmem_limit_bytes=67_043_328),
            cost_estimate=pl.CostEstimate(flops=flops, bytes_accessed=43_000_000, transcendentals=0),
        )(disp_one.reshape(split), disp_two.reshape(split), slot_one.T, slot_two.T, expert_one.T, expert_two.T,
          gate_one.T, gate_two.T, w_gate, w_up, w_down)

    in_specs = (disp_spec, tok_spec, tok_spec, tok_spec, disp_spec, tok_spec, tok_spec, tok_spec,
                weight_spec, weight_spec, weight_spec)
    return jax.shard_map(local_step, mesh=mesh, in_specs=in_specs, out_specs=(tok_spec, tok_spec), check_vma=False)
```

```python
import functools
import math

import jax
import jax.numpy as jnp
from jax import lax
from jax.experimental import pallas as pl
from jax.experimental.pallas import tpu as pltpu
from jax.sharding import PartitionSpec as P

MESH = pl.DeviceIdType.MESH
AXIS = 'expert'
CORES = 2
BF16_MAX = 3.3895313892515355e38
NT = 512
DN = 1024
LANES = 128


def moe_kernel(side, disp_one, disp_two, slot_one, slot_two, expert_one, expert_two, gate_one, gate_two, w_gate, w_up, w_down, out_one, out_two,
               wgu, wd, stage, recv, hid, own, meta, part, relay, final,
               x_sem, w_sem, d_sem, send_sem, recv_sem, meta_send, meta_recv,
               part_send, relay_recv, final_recv):
    n_exp, dim, ffn = w_gate.shape
    cap = disp_one.shape[-2]
    half = dim // 2
    tokens = out_one.shape[0]
    rows = 2 * side * CORES * cap
    group = side * CORES * n_exp * cap
    n_main = ffn // NT
    tail = ffn - n_main * NT
    routes = ((slot_one, expert_one, gate_one), (slot_two, expert_two, gate_two))
    outs = (out_one, out_two)
    top_k = slot_one.shape[0]
    top_row = 8

    me = lax.axis_index(AXIS)
    c = me % CORES
    x = (me // CORES) % side
    y = me // (CORES * side)
    turn = 1 - 2 * c

    def dev(yy, xx, cc):
        return {AXIS: ((yy % side) * side + (xx % side)) * CORES + cc % CORES}

    def along(m, first, step, dc):
        if (m == 0) == first:
            return dev(y, x + step, c + dc)
        return dev(y + step, x, c + dc)

    def rel(it):
        return (2 - it + (it // 2) * (2 * it - 1)) % side

    def load_rows(u, it, e):
        for k in range(CORES):
            r = (1 - 2 * k) * rel(it) + side
            pltpu.make_async_copy(disp_one.at[(y + r) % side, :, k, e], stage.at[u, 0, pl.ds(k * side, side)], x_sem.at[u, 0]).start()
            pltpu.make_async_copy(disp_two.at[:, (x + r) % side, k, e], stage.at[u, 1, pl.ds(k * side, side)], x_sem.at[u, 1]).start()

    def wait_rows(u):
        for m in range(2):
            pltpu.make_async_copy(stage.at[u, m], stage.at[u, m], x_sem.at[u, m]).wait()

    def load_gu(e, j, priority=0):
        width = NT if j < n_main else tail
        for k, w in enumerate((w_gate, w_up)):
            pltpu.make_async_copy(w.at[e, :, pl.ds(j * NT, width)],
                                  wgu.at[e, :, pl.ds(2 * j * NT + k * width, width)],
                                  w_sem.at[e, 2 * j + k]).start(priority=priority)

    def load_down(e, j):
        pltpu.make_async_copy(w_down.at[e, :, pl.ds(j * DN, DN)], wd.at[e, :, pl.ds(j * DN, DN)],
                              d_sem.at[e, j]).start()

    chunks = []
    for e in range(n_exp):
        chunks.append(lambda e=e: (load_rows(e, 0, e), load_gu(e, 0)))
        chunks.extend(functools.partial(load_gu, e, j) for j in range(1, n_main + 1))
        chunks.extend(functools.partial(load_down, e, j) for j in range(dim // DN))
    for it in range(1, side):
        chunks.append(lambda it=it: [load_rows(it * n_exp + e, it, e) for e in range(n_exp)])
    chunks = iter(chunks)

    def next_chunk():
        for load in chunks:
            load()
            return

    def wait_gu(e, j):
        width = NT if j < n_main else tail
        for k in range(2):
            ref = wgu.at[e, :, pl.ds(2 * j * NT + k * width, width)]
            pltpu.make_async_copy(ref, ref, w_sem.at[e, 2 * j + k]).wait()

    def wait_down(e, j):
        ref = wd.at[e, :, pl.ds(j * DN, DN)]
        pltpu.make_async_copy(ref, ref, d_sem.at[e, j]).wait()

    def hidden(j, both):
        width = NT if j < n_main else tail
        gate_act, up_act = both[:, :width], both[:, width:]
        hid[:, j * NT:j * NT + width] = (gate_act * jax.nn.sigmoid(gate_act) * up_act).astype(jnp.bfloat16)

    def put_rows(u, j, width, y_rows):
        y_rows = jnp.where(jnp.abs(y_rows) <= BF16_MAX, y_rows, 0.0).astype(jnp.bfloat16)
        stage[u, :, :, :, j * width:(j + 1) * width] = y_rows.reshape(2, CORES * side, cap, width)

    def dot(a, b):
        return jnp.dot(a, b, preferred_element_type=jnp.float32)

    def first_unit(u, e):
        wait_rows(u)
        for j in range(n_main + 1):
            width = NT if j < n_main else tail
            wait_gu(e, j)
            next_chunk()
            hidden(j, dot(stage[u].reshape(rows, dim), wgu[e, :, 2 * j * NT:2 * j * NT + 2 * width]))
        for j in range(dim // DN):
            wait_down(e, j)
            next_chunk()
            put_rows(u, j, DN, dot(hid[...], wd[e, :, j * DN:(j + 1) * DN]))

    def unit(u, e):
        wait_rows(u)
        both = dot(stage[u].reshape(rows, dim), wgu[e])
        for j in range(n_main + 1):
            width = NT if j < n_main else tail
            hidden(j, both[:, 2 * j * NT:2 * j * NT + 2 * width])
        put_rows(u, 0, dim, dot(hid[...], wd[e]))

    hops = [(2, 0), (2, 1), (1, 0), (side - 1, 0), (1, 1), (side - 1, 1), (0, 1)]

    def send_unit(u, it, e):
        for step, dc in hops:
            for m in range(2):
                pos = x if m == 0 else y
                pltpu.make_async_remote_copy(
                    src_ref=stage.at[u, m, (c + dc) % CORES * side + (pos + step) % side],
                    dst_ref=recv.at[m, it, pos, c, e],
                    send_sem=send_sem.at[u, m], recv_sem=recv_sem.at[m, it],
                    device_id=along(m, True, step, dc), device_id_type=MESH).start()
        for m in range(2):
            pos = x if m == 0 else y
            pltpu.make_async_copy(stage.at[u, m, c * side + pos], recv.at[m, it, pos, c, e], recv_sem.at[m, it]).start()

    def combine(m, it, meta_tile):
        ref = recv.at[m, it]
        pltpu.make_async_copy(ref, ref, recv_sem.at[m, it]).wait()
        lane = lax.broadcasted_iota(jnp.int32, (tokens, group), 1)
        if m == 0:
            row_id = lane + y * group
        else:
            sub = CORES * n_exp * cap
            row_id = (lane // sub) * group + x * sub + lane % sub
        row_id = row_id.astype(jnp.float32)
        table = jnp.transpose(meta_tile)
        mix = jnp.zeros((tokens, group), jnp.float32)
        for j in range(top_k):
            mix = jnp.where(table[:tokens, j:j + 1] == row_id, table[:tokens, top_row + j:top_row + j + 1], mix)
        high = mix.astype(jnp.bfloat16)
        rest = mix - high.astype(jnp.float32)
        mid = rest.astype(jnp.bfloat16)
        low = (rest - mid.astype(jnp.float32)).astype(jnp.bfloat16)
        mix3 = jnp.concatenate([high, mid, low], axis=0)
        for j in range(dim // DN):
            prod = dot(mix3, recv[m, it, :, :, :, :, j * DN:(j + 1) * DN].reshape(group, DN))
            total = prod[2 * tokens:] + prod[tokens:2 * tokens] + prod[:tokens]
            h, off = (j * DN) // half, (j * DN) % half
            part[m, it, h, :, off:off + DN] = total

    def wait_meta(m, it):
        ref = meta.at[m, it]
        pltpu.make_async_copy(ref, ref, meta_recv.at[m, it]).wait()

    next_chunk()
    next_chunk()

    barrier = pltpu.get_barrier_semaphore()
    peers = 0
    for step in range(side):
        for dc in range(CORES):
            if (step, dc) != (0, 0):
                pl.semaphore_signal(barrier, inc=1, device_id=along(0, True, step, dc), device_id_type=MESH)
                peers += 1
            if step != 0:
                pl.semaphore_signal(barrier, inc=1, device_id=along(1, True, step, dc), device_id_type=MESH)
                peers += 1

    for m, (slots, experts, gates) in enumerate(routes):
        own[m] = jnp.zeros((2 * top_row, LANES), jnp.float32)
        kept = slots[...] >= 0
        own[m, :top_k, :tokens] = jnp.where(kept, experts[...] * cap + slots[...], -1).astype(jnp.float32)
        own[m, top_row:top_row + top_k, :tokens] = gates[...]
    first_unit(0, 0)
    pl.semaphore_wait(barrier, peers)
    send_unit(0, 0, 0)
    for m in range(2):
        for it in range(side - 1):
            step = side - turn * (2, 1, 3)[it]
            pltpu.make_async_remote_copy(src_ref=own.at[m], dst_ref=meta.at[m, it], send_sem=meta_send.at[m, it],
                                         recv_sem=meta_recv.at[m, it], device_id=along(m, False, step, 0),
                                         device_id_type=MESH).start()

    for e in range(1, n_exp):
        first_unit(e, e)
        send_unit(e, 0, e)
    for _ in range(side):
        next_chunk()

    def send_far(m):
        for h, step in ((0, side + turn), (1, side - turn)):
            pltpu.make_async_remote_copy(src_ref=part.at[m, 0, h], dst_ref=relay.at[m, h],
                                         send_sem=part_send.at[m, h], recv_sem=relay_recv.at[m, h],
                                         device_id=along(m, False, step, 0), device_id_type=MESH).start()

    def send_near(m, it):
        h = it - 1
        step = side + (turn, -turn)[h]
        ref = relay.at[m, h]
        pltpu.make_async_copy(ref, ref, relay_recv.at[m, h]).wait()
        part[m, it, h] = part[m, it, h] + relay[m, h]
        pltpu.make_async_remote_copy(src_ref=part.at[m, it], dst_ref=final.at[m, h],
                                     send_sem=part_send.at[m, 2 + h], recv_sem=final_recv.at[m, h],
                                     device_id=along(m, False, step, 0), device_id_type=MESH).start()

    def body(it, carry):
        for e in range(n_exp):
            u = it * n_exp + e
            unit(u, e)
            send_unit(u, it, e)

        @pl.when(it < side - 1)
        def _():
            for m in range(2):
                @pl.when(it == 1)
                def _():
                    wait_meta(m, 0)

                @pl.when(it == 2)
                def _():
                    wait_meta(m, 1)
                combine(m, it - 1, meta[m, it - 1])

            @pl.when(it == 1)
            def _():
                for m in range(2):
                    send_far(m)

            @pl.when(it == 2)
            def _():
                for m in range(2):
                    send_near(m, 1)
        return carry

    lax.fori_loop(1, side, body, 0)
    for m in range(2):
        wait_meta(m, 2)
        combine(m, 2, meta[m, 2])
        send_near(m, 2)
    for m in range(2):
        combine(m, 3, own[m])
    for m in range(2):
        for h in range(2):
            ref = final.at[m, h]
            pltpu.make_async_copy(ref, ref, final_recv.at[m, h]).wait()
        for h in range(2):
            total = part[m, 3, h] + final[m, 0, h] + final[m, 1, h]
            outs[m][:, h * half:(h + 1) * half] = total.astype(jnp.bfloat16)

    def drain(u, carry):
        for m in range(2):
            ref = stage.at[u, m, pl.ds(0, side * CORES - 1)]
            pltpu.make_async_copy(ref, ref, send_sem.at[u, m]).wait()
        return carry

    lax.fori_loop(0, side * n_exp, drain, 0)
    for m in range(2):
        for it in range(side - 1):
            pltpu.make_async_copy(own.at[m], own.at[m], meta_send.at[m, it]).wait()
        for h in range(2):
            ref = part.at[m, 0, h]
            pltpu.make_async_copy(ref, ref, part_send.at[m, h]).wait()
            ref = part.at[m, 1 + h]
            pltpu.make_async_copy(ref, ref, part_send.at[m, 2 + h]).wait()


def copy_kernel(in_one, in_two, out_one, out_two):
    out_one[...] = in_one[...]
    out_two[...] = in_two[...]


def solution(mesh):
    members = mesh.shape[AXIS]
    side = math.isqrt(members // CORES)
    disp_spec = P('data', 'expert', None, None)
    tok_spec = P(('data', 'expert'), None)
    weight_spec = P('expert', None, None)

    def local_step(disp_one, slot_one, expert_one, gate_one, disp_two, slot_two, expert_two, gate_two, w_gate, w_up, w_down):
        _, n_exp, cap, dim = disp_one.shape
        tokens = slot_one.shape[0]
        ffn = w_gate.shape[-1]
        units = side * n_exp

        split = (side, side, CORES, n_exp, cap, dim)
        any_spec = pl.BlockSpec(memory_space=pl.ANY)
        vmem_spec = pl.BlockSpec(memory_space=pltpu.VMEM)
        dma = pltpu.SemaphoreType.DMA
        flops = 2 * 2 * members * n_exp * cap * dim * ffn * 3
        outs = pl.pallas_call(
            functools.partial(moe_kernel, side),
            out_shape=(jax.ShapeDtypeStruct((tokens, dim), jnp.bfloat16),) * 2,
            in_specs=[any_spec] * 2 + [vmem_spec] * 6 + [any_spec] * 3,
            out_specs=(vmem_spec, vmem_spec),
            scratch_shapes=[
                pltpu.VMEM((n_exp, dim, 2 * ffn), jnp.bfloat16),
                pltpu.VMEM((n_exp, ffn, dim), jnp.bfloat16),
                pltpu.VMEM((units, 2, CORES * side, cap, dim), jnp.bfloat16),
                pltpu.VMEM((2, side, side, CORES, n_exp, cap, dim), jnp.bfloat16),
                pltpu.VMEM((2 * side * CORES * cap, ffn), jnp.bfloat16),
                pltpu.VMEM((2, 16, LANES), jnp.float32),
                pltpu.VMEM((2, side - 1, 16, LANES), jnp.float32),
                pltpu.VMEM((2, side, 2, tokens, dim // 2), jnp.float32),
                pltpu.VMEM((2, 2, tokens, dim // 2), jnp.float32),
                pltpu.VMEM((2, 2, 2, tokens, dim // 2), jnp.float32),
                dma((units, 2)), dma((n_exp, 2 * (ffn // NT) + 2)), dma((n_exp, dim // DN)),
                dma((units, 2)), dma((2, side)), dma((2, side - 1)), dma((2, side - 1)),
                dma((2, 4)), dma((2, 2)), dma((2, 2)),
            ],
            compiler_params=pltpu.CompilerParams(collective_id=0, has_side_effects=True,
                                                 vmem_limit_bytes=67_043_328),
            cost_estimate=pl.CostEstimate(flops=flops, bytes_accessed=43_000_000, transcendentals=0),
        )(disp_one.reshape(split), disp_two.reshape(split), slot_one.T, slot_two.T, expert_one.T, expert_two.T,
          gate_one.T, gate_two.T, w_gate, w_up, w_down)
        return pl.pallas_call(
            copy_kernel, out_shape=(jax.ShapeDtypeStruct((tokens, dim), jnp.bfloat16),) * 2,
            in_specs=[vmem_spec, vmem_spec], out_specs=(vmem_spec, vmem_spec))(*outs)

    in_specs = (disp_spec, tok_spec, tok_spec, tok_spec, disp_spec, tok_spec, tok_spec, tok_spec,
                weight_spec, weight_spec, weight_spec)
    return jax.shard_map(local_step, mesh=mesh, in_specs=in_specs, out_specs=(tok_spec, tok_spec), check_vma=False)
```

```python
import functools
import math

import jax
import jax.numpy as jnp
from jax import lax
from jax.experimental import pallas as pl
from jax.experimental.pallas import tpu as pltpu
from jax.sharding import PartitionSpec as P

MESH = pl.DeviceIdType.MESH
AXIS = 'expert'
CORES = 2
BF16_MAX = 3.3895313892515355e38
TILES = (512, 512)
PIECE = 512
IN_FLIGHT = 9_500_000
DN = 1024
LANES = 128


def moe_kernel(side, disp_one, disp_two, slot_one, slot_two, expert_one, expert_two, gate_one, gate_two, w_gate, w_up, w_down, out_one, out_two,
               wgu, wd, stage, recv, hid, own, meta, part, relay, final,
               x_sem, w_sem, d_sem, send_sem, recv_sem, meta_send, meta_recv,
               part_send, relay_recv, final_recv):
    n_exp, dim, ffn = w_gate.shape
    cap = disp_one.shape[-2]
    half = dim // 2
    tokens = out_one.shape[0]
    rows = 2 * side * CORES * cap
    group = side * CORES * n_exp * cap
    widths = TILES + (ffn - sum(TILES),)
    starts = [sum(widths[:j]) for j in range(len(widths))]
    routes = ((slot_one, expert_one, gate_one), (slot_two, expert_two, gate_two))
    outs = (out_one, out_two)
    top_k = slot_one.shape[0]
    top_row = 8

    me = lax.axis_index(AXIS)
    c = me % CORES
    x = (me // CORES) % side
    y = me // (CORES * side)
    turn = 1 - 2 * c

    def dev(yy, xx, cc):
        return {AXIS: ((yy % side) * side + (xx % side)) * CORES + cc % CORES}

    def along(m, first, step, dc):
        if (m == 0) == first:
            return dev(y, x + step, c + dc)
        return dev(y + step, x, c + dc)

    def rel(it):
        return (2 - it + (it // 2) * (2 * it - 1)) % side

    def load_rows(u, it, e):
        for k in range(CORES):
            r = (1 - 2 * k) * rel(it) + side
            pltpu.make_async_copy(disp_one.at[(y + r) % side, :, k, e], stage.at[u, 0, pl.ds(k * side, side)], x_sem.at[u, 0]).start()
            pltpu.make_async_copy(disp_two.at[:, (x + r) % side, k, e], stage.at[u, 1, pl.ds(k * side, side)], x_sem.at[u, 1]).start()

    def wait_rows(u):
        for m in range(2):
            pltpu.make_async_copy(stage.at[u, m], stage.at[u, m], x_sem.at[u, m]).wait()

    def load_gu(e, j, off, width):
        for k, w in enumerate((w_gate, w_up)):
            pltpu.make_async_copy(w.at[e, :, pl.ds(starts[j] + off, width)],
                                  wgu.at[e, :, pl.ds(2 * starts[j] + k * widths[j] + off, width)],
                                  w_sem.at[e, j]).start()

    def load_down(e, j):
        pltpu.make_async_copy(w_down.at[e, :, pl.ds(j * DN, DN)], wd.at[e, :, pl.ds(j * DN, DN)],
                              d_sem.at[e, j]).start()

    row_bytes = 2 * rows * dim
    gu_bytes = lambda width: 2 * 2 * dim * width
    down_bytes = 2 * ffn * DN
    chunks = []
    for e in range(n_exp):
        chunks.append((row_bytes, functools.partial(load_rows, e, 0, e)))
        for j, width in enumerate(widths):
            for off in range(0, width, PIECE):
                piece = min(PIECE, width - off)
                chunks.append((gu_bytes(piece), functools.partial(load_gu, e, j, off, piece)))
        for j in range(dim // DN):
            chunks.append((down_bytes, functools.partial(load_down, e, j)))
    for it in range(1, side):
        for e in range(n_exp):
            chunks.append((row_bytes, functools.partial(load_rows, it * n_exp + e, it, e)))
    flying = [0]

    def next_chunks(done):
        flying[0] -= done
        while chunks and flying[0] + chunks[0][0] <= IN_FLIGHT:
            size, load = chunks.pop(0)
            flying[0] += size
            load()

    def wait_gu(e, j):
        ref = wgu.at[e, :, pl.ds(2 * starts[j], 2 * widths[j])]
        pltpu.make_async_copy(ref, ref, w_sem.at[e, j]).wait()

    def wait_down(e, j):
        ref = wd.at[e, :, pl.ds(j * DN, DN)]
        pltpu.make_async_copy(ref, ref, d_sem.at[e, j]).wait()

    def hidden(j, both):
        width = widths[j]
        gate_act, up_act = both[:, :width], both[:, width:]
        hid[:, starts[j]:starts[j] + width] = (gate_act * jax.nn.sigmoid(gate_act) * up_act).astype(jnp.bfloat16)

    def put_rows(u, j, width, y_rows):
        y_rows = jnp.where(jnp.abs(y_rows) <= BF16_MAX, y_rows, 0.0).astype(jnp.bfloat16)
        stage[u, :, :, :, j * width:(j + 1) * width] = y_rows.reshape(2, CORES * side, cap, width)

    def dot(a, b):
        return jnp.dot(a, b, preferred_element_type=jnp.float32)

    def first_unit(u, e, ready):
        wait_rows(u)
        done = row_bytes
        for j, width in enumerate(widths):
            wait_gu(e, j)
            next_chunks(done + gu_bytes(width))
            done = 0
            hidden(j, dot(stage[u].reshape(rows, dim), wgu[e, :, 2 * starts[j]:2 * starts[j] + 2 * width]))
        for j in range(dim // DN):
            wait_down(e, j)
            next_chunks(down_bytes)
            put_rows(u, j, DN, dot(hid[...], wd[e, :, j * DN:(j + 1) * DN]))
        ready()
        send_unit(u, 0, e)

    def unit(u, e):
        wait_rows(u)
        both = dot(stage[u].reshape(rows, dim), wgu[e])
        for j, width in enumerate(widths):
            hidden(j, both[:, 2 * starts[j]:2 * starts[j] + 2 * width])
        put_rows(u, 0, dim, dot(hid[...], wd[e]))

    hops = [(2, 0), (2, 1), (1, 0), (side - 1, 0), (1, 1), (side - 1, 1), (0, 1)]

    def send_unit(u, it, e, cols=slice(None)):
        for step, dc in hops:
            for m in range(2):
                pos = x if m == 0 else y
                pltpu.make_async_remote_copy(
                    src_ref=stage.at[u, m, (c + dc) % CORES * side + (pos + step) % side, :, cols],
                    dst_ref=recv.at[m, it, pos, c, e, :, cols],
                    send_sem=send_sem.at[u, m], recv_sem=recv_sem.at[m, it],
                    device_id=along(m, True, step, dc), device_id_type=MESH).start()
        for m in range(2):
            pos = x if m == 0 else y
            pltpu.make_async_copy(stage.at[u, m, c * side + pos, :, cols],
                                  recv.at[m, it, pos, c, e, :, cols], recv_sem.at[m, it]).start()

    def combine(m, it, meta_tile):
        ref = recv.at[m, it]
        pltpu.make_async_copy(ref, ref, recv_sem.at[m, it]).wait()
        lane = lax.broadcasted_iota(jnp.int32, (tokens, group), 1)
        if m == 0:
            row_id = lane + y * group
        else:
            sub = CORES * n_exp * cap
            row_id = (lane // sub) * group + x * sub + lane % sub
        row_id = row_id.astype(jnp.float32)
        table = jnp.transpose(meta_tile)
        mix = jnp.zeros((tokens, group), jnp.float32)
        for j in range(top_k):
            mix = jnp.where(table[:tokens, j:j + 1] == row_id, table[:tokens, top_row + j:top_row + j + 1], mix)
        high = mix.astype(jnp.bfloat16)
        rest = mix - high.astype(jnp.float32)
        mid = rest.astype(jnp.bfloat16)
        low = (rest - mid.astype(jnp.float32)).astype(jnp.bfloat16)
        mix3 = jnp.concatenate([high, mid, low], axis=0)
        for j in range(dim // DN):
            prod = dot(mix3, recv[m, it, :, :, :, :, j * DN:(j + 1) * DN].reshape(group, DN))
            total = prod[2 * tokens:] + prod[tokens:2 * tokens] + prod[:tokens]
            h, off = (j * DN) // half, (j * DN) % half
            part[m, it, h, :, off:off + DN] = total

    def wait_meta(m, it):
        ref = meta.at[m, it]
        pltpu.make_async_copy(ref, ref, meta_recv.at[m, it]).wait()

    next_chunks(0)

    barrier = pltpu.get_barrier_semaphore()
    peers = 0
    for step in range(side):
        for dc in range(CORES):
            if (step, dc) != (0, 0):
                pl.semaphore_signal(barrier, inc=1, device_id=along(0, True, step, dc), device_id_type=MESH)
                peers += 1
            if step != 0:
                pl.semaphore_signal(barrier, inc=1, device_id=along(1, True, step, dc), device_id_type=MESH)
                peers += 1

    for m, (slots, experts, gates) in enumerate(routes):
        own[m] = jnp.zeros((2 * top_row, LANES), jnp.float32)
        kept = slots[...] >= 0
        own[m, :top_k, :tokens] = jnp.where(kept, experts[...] * cap + slots[...], -1).astype(jnp.float32)
        own[m, top_row:top_row + top_k, :tokens] = gates[...]
    def meet():
        pl.semaphore_wait(barrier, peers)
        for m in range(2):
            for it in range(side - 1):
                step = side - turn * (2, 1, 3)[it]
                pltpu.make_async_remote_copy(src_ref=own.at[m], dst_ref=meta.at[m, it], send_sem=meta_send.at[m, it],
                                             recv_sem=meta_recv.at[m, it], device_id=along(m, False, step, 0),
                                             device_id_type=MESH).start()

    first_unit(0, 0, meet)
    for e in range(1, n_exp):
        first_unit(e, e, lambda: None)
    next_chunks(side * n_exp * row_bytes)

    def send_far(m):
        for h, step in ((0, side + turn), (1, side - turn)):
            pltpu.make_async_remote_copy(src_ref=part.at[m, 0, h], dst_ref=relay.at[m, h],
                                         send_sem=part_send.at[m, h], recv_sem=relay_recv.at[m, h],
                                         device_id=along(m, False, step, 0), device_id_type=MESH).start()

    def send_near(m, it):
        h = it - 1
        step = side + (turn, -turn)[h]
        ref = relay.at[m, h]
        pltpu.make_async_copy(ref, ref, relay_recv.at[m, h]).wait()
        part[m, it, h] = part[m, it, h] + relay[m, h]
        pltpu.make_async_remote_copy(src_ref=part.at[m, it], dst_ref=final.at[m, h],
                                     send_sem=part_send.at[m, 2 + h], recv_sem=final_recv.at[m, h],
                                     device_id=along(m, False, step, 0), device_id_type=MESH).start()

    def body(it, carry):
        for e in range(n_exp):
            u = it * n_exp + e
            unit(u, e)
            send_unit(u, it, e)
            if e == 0:
                @pl.when(it == 1)
                def _():
                    for m in range(2):
                        wait_meta(m, 0)
                        combine(m, 0, meta[m, 0])
                        send_far(m)

        @pl.when(it == 2)
        def _():
            for m in range(2):
                wait_meta(m, 1)
                combine(m, 1, meta[m, 1])
                send_near(m, 1)
        return carry

    lax.fori_loop(1, side, body, 0)
    for m in range(2):
        wait_meta(m, 2)
        combine(m, 2, meta[m, 2])
        send_near(m, 2)
    for m in range(2):
        combine(m, 3, own[m])
    for m in range(2):
        for h in range(2):
            ref = final.at[m, h]
            pltpu.make_async_copy(ref, ref, final_recv.at[m, h]).wait()
        for h in range(2):
            total = part[m, 3, h] + final[m, 0, h] + final[m, 1, h]
            outs[m][:, h * half:(h + 1) * half] = total.astype(jnp.bfloat16)

    def drain(u, carry):
        for m in range(2):
            ref = stage.at[u, m, pl.ds(0, side * CORES - 1)]
            pltpu.make_async_copy(ref, ref, send_sem.at[u, m]).wait()
        return carry

    lax.fori_loop(0, side * n_exp, drain, 0)
    for m in range(2):
        for it in range(side - 1):
            pltpu.make_async_copy(own.at[m], own.at[m], meta_send.at[m, it]).wait()
        for h in range(2):
            ref = part.at[m, 0, h]
            pltpu.make_async_copy(ref, ref, part_send.at[m, h]).wait()
            ref = part.at[m, 1 + h]
            pltpu.make_async_copy(ref, ref, part_send.at[m, 2 + h]).wait()


def copy_kernel(in_one, in_two, out_one, out_two):
    out_one[...] = in_one[...]
    out_two[...] = in_two[...]


def solution(mesh):
    members = mesh.shape[AXIS]
    side = math.isqrt(members // CORES)
    disp_spec = P('data', 'expert', None, None)
    tok_spec = P(('data', 'expert'), None)
    weight_spec = P('expert', None, None)

    def local_step(disp_one, slot_one, expert_one, gate_one, disp_two, slot_two, expert_two, gate_two, w_gate, w_up, w_down):
        _, n_exp, cap, dim = disp_one.shape
        tokens = slot_one.shape[0]
        ffn = w_gate.shape[-1]
        units = side * n_exp

        split = (side, side, CORES, n_exp, cap, dim)
        any_spec = pl.BlockSpec(memory_space=pl.ANY)
        vmem_spec = pl.BlockSpec(memory_space=pltpu.VMEM)
        dma = pltpu.SemaphoreType.DMA
        flops = 2 * 2 * members * n_exp * cap * dim * ffn * 3
        outs = pl.pallas_call(
            functools.partial(moe_kernel, side),
            out_shape=(jax.ShapeDtypeStruct((tokens, dim), jnp.bfloat16),) * 2,
            in_specs=[any_spec] * 2 + [vmem_spec] * 6 + [any_spec] * 3,
            out_specs=(vmem_spec, vmem_spec),
            scratch_shapes=[
                pltpu.VMEM((n_exp, dim, 2 * ffn), jnp.bfloat16),
                pltpu.VMEM((n_exp, ffn, dim), jnp.bfloat16),
                pltpu.VMEM((units, 2, CORES * side, cap, dim), jnp.bfloat16),
                pltpu.VMEM((2, side, side, CORES, n_exp, cap, dim), jnp.bfloat16),
                pltpu.VMEM((2 * side * CORES * cap, ffn), jnp.bfloat16),
                pltpu.VMEM((2, 16, LANES), jnp.float32),
                pltpu.VMEM((2, side - 1, 16, LANES), jnp.float32),
                pltpu.VMEM((2, side, 2, tokens, dim // 2), jnp.float32),
                pltpu.VMEM((2, 2, tokens, dim // 2), jnp.float32),
                pltpu.VMEM((2, 2, 2, tokens, dim // 2), jnp.float32),
                dma((units, 2)), dma((n_exp, len(TILES) + 1)), dma((n_exp, dim // DN)),
                dma((units, 2)), dma((2, side)), dma((2, side - 1)), dma((2, side - 1)),
                dma((2, 4)), dma((2, 2)), dma((2, 2)),
            ],
            compiler_params=pltpu.CompilerParams(collective_id=0, has_side_effects=True,
                                                 vmem_limit_bytes=67_043_328),
            cost_estimate=pl.CostEstimate(flops=flops, bytes_accessed=43_000_000, transcendentals=0),
        )(disp_one.reshape(split), disp_two.reshape(split), slot_one.T, slot_two.T, expert_one.T, expert_two.T,
          gate_one.T, gate_two.T, w_gate, w_up, w_down)
        return pl.pallas_call(
            copy_kernel, out_shape=(jax.ShapeDtypeStruct((tokens, dim), jnp.bfloat16),) * 2,
            in_specs=[vmem_spec, vmem_spec], out_specs=(vmem_spec, vmem_spec))(*outs)

    in_specs = (disp_spec, tok_spec, tok_spec, tok_spec, disp_spec, tok_spec, tok_spec, tok_spec,
                weight_spec, weight_spec, weight_spec)
    return jax.shard_map(local_step, mesh=mesh, in_specs=in_specs, out_specs=(tok_spec, tok_spec), check_vma=False)
```
